32 devices in a mesh: group: 4 (over y, core), shard: 8 (over z, x).
Axes of the slice: x: 2, y: 2, z: 4, core: 2. Of those that a mesh axis runs over, the one named last changes fastest.
Arguments:
- params: float32 [512, 7168], P(('group', 'shard')), may hold values from -3 to 3
- gradient: bfloat16 [512, 7168], P(('group', 'shard'))
- first_moment: float32 [512, 7168], P(('group', 'shard')), may hold values from -2 to 2
- second_moment: float32 [512, 7168], P(('group', 'shard')), may hold values from 0.01 to 1
Outputs:
- new_params: float32 [512, 7168], P(('group', 'shard'))
- new_first: float32 [512, 7168], P(('group', 'shard'))
- new_second: float32 [512, 7168], P(('group', 'shard'))
- replica: bfloat16 [512, 7168], P('group')
The draws below stay inside these ranges and needn't reach their ends.
All inputs are finite; a program needn't handle non-finite values.
Results may differ from the reference program's by a relative error of at most 0.00055.
Values may be sent and summed in bfloat16 or wider, within the bound.
No kernel may reach another device: no remote copies, remote signals or barrier semaphores. Data moves between devices by JAX's collectives and lax.ppermute only.
A program may use at most 64 MiB of HBM per device.

```python
import math
import jax
import jax.numpy as jnp

D = 7168
ROWS = 512


def draw_gradient(key, part):
    key_noise, key_rows, key_cols = jax.random.split(key, 3)
    row_index = jnp.arange(ROWS, dtype=jnp.float32)
    row_ramp = 1.0 + 2.0 * row_index / max(ROWS - 1, 1)
    row_rough = jnp.exp(jax.random.uniform(key_rows, (ROWS,), jnp.float32, 0.0, math.log(10.0)))
    col_rough = jnp.exp(jax.random.uniform(key_cols, (D,), jnp.float32, 0.0, math.log(10.0)))
    base_noise = jax.random.normal(key_noise, (ROWS, D), jnp.float32)
    values = 0.1 * base_noise * (row_ramp * row_rough)[:, None] * col_rough[None, :]
    return values.astype(jnp.bfloat16)


def level_of(own_key, dims, shards, smallest, largest):
    def one(position, blocks):
        heights = jax.random.uniform(jax.random.fold_in(jax.random.fold_in(own_key, 6), position), (blocks,), jnp.float32, smallest / len(shards), largest / len(shards))
        return jnp.repeat(jnp.exp(heights), dims[position] // blocks).reshape((-1,) + (1,) * (len(dims) - position - 1))

    factor_of = one(*shards[0])
    for cut in shards[1:]:
        factor_of = factor_of * one(*cut)
    return factor_of


def scatter_about(rng, dims, spread, reach, cuts=(), kind=jnp.bfloat16):
    result = jax.random.normal(rng, dims, jnp.float32) * spread
    if len(cuts) > 0:
        result = level_of(rng, dims, cuts, -0.22, 0.18) * result
    return jnp.clip(result, min=-reach, max=reach).astype(kind)


def setup_inputs(seed: int = 0) -> dict:
    keys = jax.random.split(jax.random.key(seed), 5)
    params = scatter_about(keys[0], (ROWS, D), 0.5, 3.0, ((0, 32),), jnp.float32)
    gradient = draw_gradient(jax.random.fold_in(keys[4], 71), 0)
    first_moment = scatter_about(keys[2], (ROWS, D), 0.3, 2.0, ((0, 32),), jnp.float32)
    second_moment = jnp.clip(jnp.exp(math.log(1.0) - 4.6051702 * jax.random.uniform(keys[3], (ROWS, D), jnp.float32) ** level_of(keys[3], (ROWS, D), ((0, 32),), -0.2, 0.2)), 0.01, 1.0)
    return {"params": params, "gradient": gradient, "first_moment": first_moment, "second_moment": second_moment}


def reference(params, gradient, first_moment, second_moment):
    grad_full = gradient.astype(jnp.float32)
    norm_total = jnp.sum(grad_full * grad_full)
    clip_scale = jnp.minimum(jnp.float32(1.0), 1.0 / jnp.sqrt(norm_total / (ROWS * D) + 1e-06))
    clipped = clip_scale * grad_full
    new_first = 0.9 * first_moment + 0.1 * clipped
    new_second = 0.95 * second_moment + 0.05 * clipped * clipped
    correct_one = 1.0 - 0.9 ** 10
    correct_two = 1.0 - 0.95 ** 10
    advance = new_first / correct_one / (jnp.sqrt(new_second / correct_two) + 1e-08)
    new_params = params - 0.1 * (advance + 0.1 * params)
    return (new_params, new_first, new_second, new_params.astype(jnp.bfloat16))
```

```python
import functools
import jax
import jax.numpy as jnp
from jax import lax
from jax.experimental import pallas as pl
from jax.experimental.pallas import tpu as pltpu
from jax.sharding import PartitionSpec as P

LANES = 128
VLIMIT = 8 << 20


def vmem(shape, dtype):
    return pltpu.VMEM(shape, dtype)


def pinned(x):
    return pltpu.with_memory_space_constraint(x, pltpu.VMEM)


V = pl.BlockSpec(memory_space=pltpu.VMEM)
ANY = pl.BlockSpec(memory_space=pl.ANY)


def load_kernel(g_hbm, part, g, sem):
    copy = pltpu.make_async_copy(g_hbm, g, sem)
    copy.start()
    copy.wait()
    rows, cols = g.shape
    acc = jnp.zeros((rows, LANES), jnp.float32)
    for j in range(cols // LANES):
        x = g[:, j * LANES:(j + 1) * LANES].astype(jnp.float32)
        acc = acc + x * x
    total = jnp.sum(acc, axis=0, keepdims=True)
    part[...] = jnp.broadcast_to(total, part.shape)


def update_kernel(entries, parts, g, p, m, v, new_p, new_m, new_v, top, bottom):
    norm_total = jnp.sum(parts[...])
    base = jnp.full((1, LANES), norm_total / entries + 1e-06, jnp.float32)
    clip_scale = jnp.minimum(jnp.float32(1.0), lax.rsqrt(base))
    correct_one = 1.0 - 0.9**10
    correct_two = 1.0 - 0.95**10
    rows, cols = g.shape
    half = rows // 2
    for j in range(cols // LANES):
        s = slice(j * LANES, (j + 1) * LANES)
        clipped = clip_scale * g[:, s].astype(jnp.float32)
        first = 0.9 * m[:, s] + 0.1 * clipped
        second = 0.95 * v[:, s] + 0.05 * clipped * clipped
        stepped = first / correct_one / (jnp.sqrt(second / correct_two) + 1e-08)
        value = p[:, s] - 0.1 * (stepped + 0.1 * p[:, s])
        new_m[:, s] = first
        new_v[:, s] = second
        new_p[:, s] = value
        rounded = value.astype(jnp.bfloat16)
        top[:, s] = rounded[:half]
        bottom[:, s] = rounded[half:]


def flush_kernel(n_in, *refs):
    ins, outs, sems = refs[:n_in], refs[n_in:-1], refs[-1]
    copies = [pltpu.make_async_copy(s, d, sems.at[i]) for i, (s, d) in enumerate(zip(ins, outs))]
    for c in copies:
        c.start()
    for c in copies:
        c.wait()


class Cycle:
    def __init__(self, mesh):
        self.n = mesh.shape["shard"]
        line = mesh.devices.reshape(mesh.shape["group"], self.n)[0]
        rows = cols = 1
        coords = [getattr(d, "coords", None) for d in line]
        if None not in coords:
            first = coords[0]
            cols = next((i for i in range(1, self.n) if sum(a != b for a, b in zip(coords[i], coords[i - 1])) > 1), self.n)
            rows = self.n // cols
        if rows * cols != self.n or rows % 2 or cols < 2:
            rows, cols = self.n, 1
        self.rows, self.cols = rows, cols

    def at(self, q):
        w = self.cols - 1
        if w == 0:
            return q
        turn = self.rows * w
        if isinstance(q, int):
            if q >= turn:
                return (self.rows - 1 - (q - turn)) * self.cols
            r, t = divmod(q, w)
            return r * self.cols + (t + 1 if r % 2 == 0 else w - t)
        r, t = q // w, lax.rem(q, w)
        out = r * self.cols + jnp.where(lax.rem(r, 2) == 0, t + 1, w - t)
        return jnp.where(q >= turn, (self.rows - 1 - (q - turn)) * self.cols, out)

    def place(self, s):
        w = self.cols - 1
        if w == 0:
            return s
        r, c = s // self.cols, lax.rem(s, self.cols)
        out = r * w + jnp.where(lax.rem(r, 2) == 0, c - 1, w - c)
        return jnp.where(c == 0, self.rows * w + (self.rows - 1 - r), out)

    def steps(self, by):
        return [(self.at(q), self.at((q + by) % self.n)) for q in range(self.n)]


def place_kernel(cycle, items, chained, *refs):
    chunks, out, sems = refs[:len(items)], refs[-2], refs[-1]
    here = cycle.place(lax.axis_index("shard"))
    copies = []
    for i, (hops, half) in enumerate(items):
        depth = chunks[i].shape[0]
        block = cycle.at(lax.rem(here - hops + 2 * cycle.n, cycle.n))
        row = pl.multiple_of((2 * block + half) * depth, depth)
        copies.append(pltpu.make_async_copy(chunks[i], out.at[pl.ds(row, depth)], sems.at[i]))
    for c in copies:
        c.start()
    for c in copies:
        c.wait()


def place(cycle, items, chunks, shape, out=None):
    chained = out is not None
    args = [pinned(c) for c in chunks] + ([out] if chained else [])
    return pl.pallas_call(
        functools.partial(place_kernel, cycle, items, chained),
        out_shape=jax.ShapeDtypeStruct(shape, chunks[0].dtype),
        in_specs=[V] * len(chunks) + [ANY] * chained,
        out_specs=ANY,
        scratch_shapes=[pltpu.SemaphoreType.DMA((len(chunks),))],
        input_output_aliases={len(chunks): 0} if chained else {},
        compiler_params=pltpu.CompilerParams(vmem_limit_bytes=VLIMIT),
        name="place",
    )(*args)


def on_device(cycle, n_all, params, gradient, first_moment, second_moment):
    rows, cols = gradient.shape
    f32, bf16 = jnp.float32, jnp.bfloat16
    big = vmem((rows, cols), f32)
    half = vmem((rows // 2, cols), bf16)
    part, g = pl.pallas_call(
        load_kernel,
        out_shape=(vmem((n_all, LANES), f32), vmem((rows, cols), bf16)),
        in_specs=[ANY],
        out_specs=(V,) * 2,
        scratch_shapes=[pltpu.SemaphoreType.DMA],
        compiler_params=pltpu.CompilerParams(vmem_limit_bytes=VLIMIT),
        name="load",
    )(pltpu.with_memory_space_constraint(gradient, pltpu.HBM))
    parts = lax.all_to_all(part.reshape(n_all, 1, LANES), ("group", "shard"), 0, 0, tiled=True).reshape(n_all, LANES)
    entries = rows * cols * n_all
    new_p, new_m, new_v, top, bottom = pl.pallas_call(
        functools.partial(update_kernel, entries),
        out_shape=(big, big, big, half, half),
        in_specs=[V] * 5,
        out_specs=(V,) * 5,
        compiler_params=pltpu.CompilerParams(vmem_limit_bytes=VLIMIT),
        name="update",
    )(pinned(parts), *(pinned(a) for a in (g, params, first_moment, second_moment)))
    new_p, new_m, new_v = pl.pallas_call(
        functools.partial(flush_kernel, 3),
        out_shape=(jax.ShapeDtypeStruct((rows, cols), f32),) * 3,
        in_specs=[V] * 3,
        out_specs=(ANY,) * 3,
        scratch_shapes=[pltpu.SemaphoreType.DMA((3,))],
        compiler_params=pltpu.CompilerParams(vmem_limit_bytes=VLIMIT),
        name="flush",
    )(pinned(new_p), pinned(new_m), pinned(new_v))

    n = cycle.n
    forward, backward = cycle.steps(1), cycle.steps(-1)
    got = {(0, 0): top, (0, 1): bottom}
    up, down = [top, bottom], [top, bottom]
    far, near = n // 2, (n - 1) // 2
    order = []
    for k in range(1, far + 1):
        for half_of, hops, reach in ((0, k, far), (1, -k, far), (1, k, near), (0, -k, near)):
            if k > reach:
                continue
            held, pairs = (up, forward) if hops > 0 else (down, backward)
            held[half_of] = lax.ppermute(held[half_of], "shard", pairs)
            got[hops, half_of] = held[half_of]
            order.append((hops, half_of))
    shape = (n * rows, cols)
    early = [(0, 0), (0, 1)] + order[:-6]
    late = order[-6:]
    replica = place(cycle, early, [got[i] for i in early], shape)
    replica = place(cycle, late, [got[i] for i in late], shape, replica)
    return new_p, new_m, new_v, replica


def solution(mesh):
    rows = P(("group", "shard"), None)
    return jax.shard_map(
        functools.partial(on_device, Cycle(mesh), mesh.shape["group"] * mesh.shape["shard"]),
        mesh=mesh,
        in_specs=(rows,) * 4,
        out_specs=(rows,) * 3 + (P("group", None),),
        check_vma=False,
    )
```

```python
import functools
import jax
import jax.numpy as jnp
from jax import lax
from jax.experimental import pallas as pl
from jax.experimental.pallas import tpu as pltpu
from jax.sharding import PartitionSpec as P

LANES = 128
VLIMIT = 8 << 20


def vmem(shape, dtype):
    return pltpu.VMEM(shape, dtype)


def pinned(x):
    return pltpu.with_memory_space_constraint(x, pltpu.VMEM)


V = pl.BlockSpec(memory_space=pltpu.VMEM)
ANY = pl.BlockSpec(memory_space=pl.ANY)


def load_kernel(g_hbm, p_hbm, m_hbm, v_hbm, part, g, p, m, v, sems):
    copies = [
        pltpu.make_async_copy(s, d, sems.at[i])
        for i, (s, d) in enumerate(((g_hbm, g), (p_hbm, p), (m_hbm, m), (v_hbm, v)))
    ]
    for c in copies:
        c.start()
    copies[0].wait()
    rows, cols = g.shape
    accs = [jnp.zeros((rows, LANES), jnp.float32) for _ in range(4)]
    for j in range(cols // LANES):
        x = g[:, j * LANES:(j + 1) * LANES].astype(jnp.float32)
        accs[j % 4] = accs[j % 4] + x * x
    total = jnp.sum((accs[0] + accs[1]) + (accs[2] + accs[3]), axis=0, keepdims=True)
    part[...] = jnp.broadcast_to(total, part.shape)
    for c in copies[1:]:
        c.wait()


def update_kernel(entries, parts, g, p, m, v, new_p, new_m, new_v, top, bottom):
    norm_total = jnp.sum(parts[...])
    base = jnp.full((1, LANES), norm_total / entries + 1e-06, jnp.float32)
    clip_scale = jnp.minimum(jnp.float32(1.0), lax.rsqrt(base))
    correct_one = 1.0 - 0.9**10
    correct_two = 1.0 - 0.95**10
    rows, cols = g.shape
    half = rows // 2
    for j in range(cols // LANES):
        s = slice(j * LANES, (j + 1) * LANES)
        clipped = clip_scale * g[:, s].astype(jnp.float32)
        first = 0.9 * m[:, s] + 0.1 * clipped
        second = 0.95 * v[:, s] + 0.05 * clipped * clipped
        stepped = first / correct_one / (jnp.sqrt(second / correct_two) + 1e-08)
        value = p[:, s] - 0.1 * (stepped + 0.1 * p[:, s])
        new_m[:, s] = first
        new_v[:, s] = second
        new_p[:, s] = value
        rounded = value.astype(jnp.bfloat16)
        top[:, s] = rounded[:half]
        bottom[:, s] = rounded[half:]


def flush_kernel(n_in, *refs):
    ins, outs, sems = refs[:n_in], refs[n_in:-1], refs[-1]
    copies = [pltpu.make_async_copy(s, d, sems.at[i]) for i, (s, d) in enumerate(zip(ins, outs))]
    for c in copies:
        c.start()
    for c in copies:
        c.wait()


class Cycle:
    def __init__(self, mesh):
        self.n = mesh.shape["shard"]
        line = mesh.devices.reshape(mesh.shape["group"], self.n)[0]
        rows = cols = 1
        coords = [getattr(d, "coords", None) for d in line]
        if None not in coords:
            first = coords[0]
            cols = next((i for i in range(1, self.n) if sum(a != b for a, b in zip(coords[i], coords[i - 1])) > 1), self.n)
            rows = self.n // cols
        if rows * cols != self.n or rows % 2 or cols < 2:
            rows, cols = self.n, 1
        self.rows, self.cols = rows, cols

    def at(self, q):
        w = self.cols - 1
        if w == 0:
            return q
        turn = self.rows * w
        if isinstance(q, int):
            if q >= turn:
                return (self.rows - 1 - (q - turn)) * self.cols
            r, t = divmod(q, w)
            return r * self.cols + (t + 1 if r % 2 == 0 else w - t)
        r, t = q // w, lax.rem(q, w)
        out = r * self.cols + jnp.where(lax.rem(r, 2) == 0, t + 1, w - t)
        return jnp.where(q >= turn, (self.rows - 1 - (q - turn)) * self.cols, out)

    def place(self, s):
        w = self.cols - 1
        if w == 0:
            return s
        r, c = s // self.cols, lax.rem(s, self.cols)
        out = r * w + jnp.where(lax.rem(r, 2) == 0, c - 1, w - c)
        return jnp.where(c == 0, self.rows * w + (self.rows - 1 - r), out)

    def steps(self, by):
        return [(self.at(q), self.at((q + by) % self.n)) for q in range(self.n)]


def place_kernel(cycle, items, chained, *refs):
    chunks, out, sems = refs[:len(items)], refs[-2], refs[-1]
    here = cycle.place(lax.axis_index("shard"))
    copies = []
    for i, (hops, half) in enumerate(items):
        depth = chunks[i].shape[0]
        block = cycle.at(lax.rem(here - hops + 2 * cycle.n, cycle.n))
        row = pl.multiple_of((2 * block + half) * depth, depth)
        copies.append(pltpu.make_async_copy(chunks[i], out.at[pl.ds(row, depth)], sems.at[i]))
    for c in copies:
        c.start()
    for c in copies:
        c.wait()


def place(cycle, items, chunks, shape, out=None):
    chained = out is not None
    args = [pinned(c) for c in chunks] + ([out] if chained else [])
    return pl.pallas_call(
        functools.partial(place_kernel, cycle, items, chained),
        out_shape=jax.ShapeDtypeStruct(shape, chunks[0].dtype),
        in_specs=[V] * len(chunks) + [ANY] * chained,
        out_specs=ANY,
        scratch_shapes=[pltpu.SemaphoreType.DMA((len(chunks),))],
        input_output_aliases={len(chunks): 0} if chained else {},
        compiler_params=pltpu.CompilerParams(vmem_limit_bytes=VLIMIT),
        name="place",
    )(*args)


def on_device(cycle, n_all, params, gradient, first_moment, second_moment):
    rows, cols = gradient.shape
    f32, bf16 = jnp.float32, jnp.bfloat16
    big = vmem((rows, cols), f32)
    half = vmem((rows // 2, cols), bf16)
    part, g, p, m, v = pl.pallas_call(
        load_kernel,
        out_shape=(vmem((n_all, LANES), f32), vmem((rows, cols), bf16), big, big, big),
        in_specs=[ANY] * 4,
        out_specs=(V,) * 5,
        scratch_shapes=[pltpu.SemaphoreType.DMA((4,))],
        compiler_params=pltpu.CompilerParams(vmem_limit_bytes=VLIMIT),
        name="load",
    )(*(pltpu.with_memory_space_constraint(a, pltpu.HBM) for a in (gradient, params, first_moment, second_moment)))
    parts = lax.all_to_all(part.reshape(n_all, 1, LANES), ("group", "shard"), 0, 0, tiled=True).reshape(n_all, LANES)
    entries = rows * cols * n_all
    new_p, new_m, new_v, top, bottom = pl.pallas_call(
        functools.partial(update_kernel, entries),
        out_shape=(big, big, big, half, half),
        in_specs=[V] * 5,
        out_specs=(V,) * 5,
        compiler_params=pltpu.CompilerParams(vmem_limit_bytes=VLIMIT),
        name="update",
    )(pinned(parts), *(pinned(a) for a in (g, p, m, v)))
    new_p, new_m, new_v = pl.pallas_call(
        functools.partial(flush_kernel, 3),
        out_shape=(jax.ShapeDtypeStruct((rows, cols), f32),) * 3,
        in_specs=[V] * 3,
        out_specs=(ANY,) * 3,
        scratch_shapes=[pltpu.SemaphoreType.DMA((3,))],
        compiler_params=pltpu.CompilerParams(vmem_limit_bytes=VLIMIT),
        name="flush",
    )(pinned(new_p), pinned(new_m), pinned(new_v))

    n = cycle.n
    forward, backward = cycle.steps(1), cycle.steps(-1)
    got = {(0, 0): top, (0, 1): bottom}
    up, down = [top, bottom], [top, bottom]
    far, near = n // 2, (n - 1) // 2
    order = []
    for k in range(1, far + 1):
        for half_of, hops, reach in ((0, k, far), (1, -k, far), (1, k, near), (0, -k, near)):
            if k > reach:
                continue
            held, pairs = (up, forward) if hops > 0 else (down, backward)
            held[half_of] = lax.ppermute(held[half_of], "shard", pairs)
            got[hops, half_of] = held[half_of]
            order.append((hops, half_of))
    shape = (n * rows, cols)
    early = [(0, 0), (0, 1)] + order[:-6]
    late = order[-6:]
    replica = place(cycle, early, [got[i] for i in early], shape)
    replica = place(cycle, late, [got[i] for i in late], shape, replica)
    return new_p, new_m, new_v, replica


def solution(mesh):
    rows = P(("group", "shard"), None)
    return jax.shard_map(
        functools.partial(on_device, Cycle(mesh), mesh.shape["group"] * mesh.shape["shard"]),
        mesh=mesh,
        in_specs=(rows,) * 4,
        out_specs=(rows,) * 3 + (P("group", None),),
        check_vma=False,
    )
```
